32 devices in a mesh: tm: 2 (over core), space: 16 (over z, y, x).
Axes of the slice: x: 2, y: 2, z: 4, core: 2. Of those that a mesh axis runs over, the one named last changes fastest.
Arguments:
- checkpoints: float32 [2, 5, 2048, 128], P('tm', None, 'space'), may hold values from -6 to 6
- sources: float32 [2, 5, 2048, 128], P(None, None, 'space'), may hold values from -3 to 3
- pitch: float32 [8], replicated, may hold values from -3.140625 to 3.140625
- metric: float32 [2048, 128], P('space'), may hold values from 0.5 to 2
- obj_weight: float32 [5, 2048, 128], P(None, 'space'), may hold values from 0.1 to 0.6
- adjoint_end: float32 [5, 2048, 128], P(None, 'space'), may hold values from -6 to 6
- lift: bfloat16 [5, 128, 128], replicated, may hold values from -0.5 to 0.5
- mixing: float32 [5, 5, 5], replicated, may hold values from -1.25 to 1.25
- faces: int32 [2048, 4], P('space'), may hold values from 0 to 191
- send_idx: int32 [16, 4, 16], P('space'), may hold values from 0 to 127
Outputs:
- adjoint_bounds: float32 [2, 5, 2048, 128], P('tm', None, 'space')
- pitch_grad: float32 [8], replicated
The draws below stay inside these ranges and needn't reach their ends.
Inputs may be any that keep to these rules, and one draw needn't show every extreme that they name: `faces`: values below 128 name the subdomain's own blocks; value 128 + d * 16 + s names slot s of the blocks received from direction d. `send_idx`: entry [p, d, s] is a local block of subdomain p sent to subdomain p + o[d], o = (1, -1, 2, -2); blocks may repeat.
All inputs are finite; a program needn't handle non-finite values.
Results may differ from the reference program's by a relative error of at most 0.0035.
Values may be sent and summed in bfloat16 or wider, within the bound.
A program may use at most 64 MiB of HBM per device.

```python
import math
import jax
import jax.numpy as jnp
from jax import lax

COMPS = 5
NODES = 128
FACES = 4
LEVELS = 8
BLK_DEV = 128
HALO = 16
NBT = 2048
N_TM = 2
N_SPACE = 16


def with_ends(drawn, key, least, high):
    extent = drawn.shape
    spot = [jax.random.randint(jax.random.fold_in(key, axis), (), 0, extent[axis]) for axis in range(len(extent))]
    drawn = drawn.at[tuple(spot)].set(least)
    longest = extent.index(max(extent))
    spot[longest] = (spot[longest] + 1) % extent[longest]
    return drawn.at[tuple(spot)].set(high)


def level_of(rng, extent, cuts, low, largest):
    factor_of, own = 1.0, jax.random.fold_in(rng, 6)
    for position, blocks in cuts:
        steps = jnp.exp(jax.random.uniform(jax.random.fold_in(own, position), (blocks,), jnp.float32, low / len(cuts), largest / len(cuts)))
        factor_of = factor_of * jnp.repeat(steps, extent[position] // blocks).reshape([-1 if axis == position else 1 for axis in range(len(extent))])
    return factor_of


def noise(rng, dims, spread, limit, cuts=(), held_as=jnp.bfloat16):
    entries = jax.random.normal(rng, dims, jnp.float32) * spread
    if len(cuts) > 0:
        entries = level_of(rng, dims, cuts, -0.22, 0.18) * entries
    return jnp.clip(entries, min=-limit, max=limit).astype(held_as)


def setup_inputs(seed: int = 0) -> dict:
    key_of = jax.random.split(jax.random.key(seed), 11)
    return {
        "checkpoints": noise(key_of[0], (2, COMPS, NBT, NODES), 1.0, 6.0, ((0, 2), (2, 16)), jnp.float32),
        "sources": noise(key_of[1], (2, COMPS, NBT, NODES), 0.5, 3.0, ((2, 16),), jnp.float32),
        "pitch": jnp.clip(jax.random.uniform(key_of[2], (LEVELS,), jnp.float32, -3.140625, 3.140625), -3.140625, 3.140625),
        "metric": jnp.clip(jnp.exp(math.log(2.0) - 1.3862944 * jax.random.uniform(key_of[3], (NBT, NODES), jnp.float32) ** level_of(key_of[3], (NBT, NODES), ((0, 16),), -0.2, 0.2)), 0.5, 2.0),
        "obj_weight": jnp.clip(0.1 + 0.5 * jax.random.uniform(key_of[4], (COMPS, NBT, NODES), jnp.float32) ** level_of(key_of[4], (COMPS, NBT, NODES), ((1, 16),), -0.2, 0.2), 0.1, 0.6),
        "adjoint_end": noise(key_of[5], (COMPS, NBT, NODES), 1.0, 6.0, ((1, 16),), jnp.float32),
        "lift": noise(key_of[6], (FACES + 1, NODES, NODES), NODES ** -0.5, 0.5),
        "mixing": noise(key_of[7], (FACES + 1, COMPS, COMPS), (COMPS * (FACES + 1)) ** -0.5, 1.25, (), jnp.float32),
        "faces": with_ends(jax.random.randint(key_of[8], (NBT, FACES), 0, BLK_DEV + 4 * HALO), jax.random.fold_in(key_of[8], 1), 0, (BLK_DEV + 4 * HALO) - 1).astype(jnp.int32),
        "send_idx": with_ends(jax.random.randint(key_of[9], (N_SPACE, 4, HALO), 0, BLK_DEV), jax.random.fold_in(key_of[9], 1), 0, BLK_DEV - 1).astype(jnp.int32),
    }


OFFSETS = (1, -1, 2, -2)
STEP_SIZE = 0.5

def global_faces(faces, send_idx):
    total_blocks = faces.shape[0]
    blk_count = total_blocks // N_SPACE
    slot_count = send_idx.shape[2]
    owner_dev = (jnp.arange(total_blocks, dtype=jnp.int32) // blk_count)[:, None]
    inside = owner_dev * blk_count + faces
    beyond = jnp.maximum(faces - blk_count, 0)
    direction = beyond // slot_count
    slot_pos = beyond % slot_count
    shifts = jnp.array(OFFSETS, dtype=jnp.int32)[direction]
    source_dev = owner_dev - shifts
    is_valid = (source_dev >= 0) & (source_dev < N_SPACE)
    clipped = jnp.clip(source_dev, 0, N_SPACE - 1)
    flat_send = send_idx.reshape(-1)
    picked = flat_send[(clipped * 4 + direction) * slot_count + slot_pos]
    outside = jnp.where(is_valid, clipped * blk_count + picked, total_blocks)
    return jnp.where(faces < blk_count, inside, outside).astype(jnp.int32)

def residual_of(current, global_index, metric, lift_float, mixing):
    squashed = lax.optimization_barrier(jnp.tanh(current).astype(jnp.bfloat16))
    squashed = squashed.astype(jnp.float32)
    padded = jnp.concatenate([squashed, jnp.zeros((COMPS, 1, NODES), jnp.float32)], axis=1)
    totals = jnp.zeros(current.shape, jnp.float32)
    for face_slot in range(global_index.shape[1]):
        picked = padded[:, global_index[:, face_slot], :]
        products = jnp.einsum('cbj,ij->cbi', picked, lift_float[face_slot], precision=lax.Precision.HIGHEST)
        totals = totals + jnp.einsum('ec,cbi->ebi', mixing[face_slot], products, precision=lax.Precision.HIGHEST)
    return metric[None] * totals

def transpose_of(adjoint, current, global_index, metric, lift_float, mixing):
    total_blocks = current.shape[1]
    weighted = metric[None] * adjoint
    totals = jnp.zeros((COMPS, total_blocks + 1, NODES), jnp.float32)
    for face_slot in range(global_index.shape[1]):
        mixed = jnp.einsum('ec,ebi->cbi', mixing[face_slot], weighted, precision=lax.Precision.HIGHEST)
        mixed = lax.optimization_barrier(mixed.astype(jnp.bfloat16)).astype(jnp.float32)
        returned_terms = jnp.einsum('cbi,ij->cbj', mixed, lift_float[face_slot], precision=lax.Precision.HIGHEST)
        totals = totals.at[:, global_index[:, face_slot], :].add(returned_terms)
    derivative = 1.0 - jnp.tanh(current) ** 2
    return totals[:, :total_blocks, :] * derivative

def reference(checkpoints, sources, pitch, metric, obj_weight, adjoint_end, lift, mixing, faces, send_idx):
    total_blocks = faces.shape[0]
    own_index = jnp.arange(total_blocks, dtype=jnp.int32)[:, None]
    global_index = jnp.concatenate([own_index, global_faces(faces, send_idx)], axis=1).astype(jnp.int32)
    half_count = LEVELS // N_TM
    lift_float = lift.astype(jnp.float32)
    states = []
    current = checkpoints[0]
    for segment in range(N_TM):
        current = checkpoints[segment]
        for within in range(half_count):
            level_now = segment * half_count + within
            states.append(current)
            forcing = jnp.cos(pitch[level_now]) * sources[0] + jnp.sin(pitch[level_now]) * sources[1]
            current = current + STEP_SIZE * (forcing - residual_of(current, global_index, metric, lift_float, mixing))
    states.append(current)
    normalizer = math.sqrt(COMPS * NODES * total_blocks)
    adjoint = adjoint_end + obj_weight * states[LEVELS]
    grads = [None] * LEVELS
    bounds = [None, None]
    for level_now in reversed(range(LEVELS)):
        turning = jnp.cos(pitch[level_now]) * sources[1] - jnp.sin(pitch[level_now]) * sources[0]
        grads[level_now] = STEP_SIZE * jnp.sum(adjoint * turning) / normalizer
        adjoint = adjoint - STEP_SIZE * transpose_of(adjoint, states[level_now], global_index, metric, lift_float, mixing)
        if level_now > 0:
            adjoint = adjoint + obj_weight * states[level_now]
        if level_now % half_count == 0:
            bounds[level_now // half_count] = adjoint
    return (jnp.stack(bounds), jnp.stack(grads))
```

```python
import functools
import math

import jax
import jax.numpy as jnp
from jax import lax
from jax.experimental import pallas as pl
from jax.experimental.pallas import tpu as pltpu
from jax.sharding import PartitionSpec as P

OFFSETS = (1, -1, 2, -2)
STEP_SIZE = 0.5
F32 = jnp.float32
BF16 = jnp.bfloat16
MESH = pl.DeviceIdType.MESH


def dot(a, b):
    return jnp.dot(a, b, preferred_element_type=F32)


def window_kernel(
    dims,
    pitch_ref, mixing_ref, cp_hbm, src_hbm, metric_hbm, weight_hbm, end_hbm, lift_ref, faces_ref, send_ref,
    out_ref, grad_ref,
    u_ref, src_ref, metric_ref, weight_ref, a_ref, hand_ref, base_ref, dd_ref, wu_ref, lift_t, sq_ref,
    p_own, p_halo, pt_own, pt_halo, pick, pick_t, out_buf, in_buf, back_out, back_in, y_ref, yh_ref, z_ref,
    mixed_ref, g_ref, gw_ref, gh_ref, row_ref, rows_ref,
    load_sems, send_sems, recv_sems, bsend_sems, brecv_sems, hand_sems, gsend_sems, grecv_sems,
):
    comps, blocks, nodes, slots, halo, half, n_tm, n_space, norm = dims
    ghosts = 4 * halo
    faces_n = slots - 1
    wide = comps * nodes
    tm = lax.axis_index("tm")
    sp = lax.axis_index("space")
    n_dev = n_tm * n_space
    me = tm * n_space + sp

    loads = [
        pltpu.make_async_copy(cp_hbm.at[0], u_ref, load_sems.at[0]),
        pltpu.make_async_copy(src_hbm, src_ref, load_sems.at[1]),
        pltpu.make_async_copy(metric_hbm, metric_ref, load_sems.at[2]),
        pltpu.make_async_copy(weight_hbm, weight_ref, load_sems.at[3]),
        pltpu.make_async_copy(end_hbm, a_ref, load_sems.at[4]),
    ]
    for load in loads:
        load.start()

    in_buf[...] = jnp.zeros_like(in_buf)
    back_in[...] = jnp.zeros_like(back_in)

    barrier = pltpu.get_barrier_semaphore()

    def greet(r, carry):
        other = lax.rem(me + r, n_dev)
        pl.semaphore_signal(
            barrier, inc=1, device_id=(other // n_space, lax.rem(other, n_space)), device_id_type=MESH
        )
        return carry

    lax.fori_loop(1, n_dev, greet, 0)

    row_ids = lax.broadcasted_iota(jnp.int32, (blocks, blocks), 0)
    lane_ids = lax.broadcasted_iota(jnp.int32, (blocks, blocks), 1)
    face_cols = []
    for k in range(faces_n):
        col = jnp.broadcast_to(faces_ref[:, k : k + 1], (blocks, blocks))
        face_cols.append(col)
        p_own[k * blocks : (k + 1) * blocks, :] = (col == lane_ids).astype(F32).astype(BF16)
        turned = jnp.transpose(col.astype(F32)).astype(jnp.int32)
        pt_own[k * blocks : (k + 1) * blocks, :] = (turned == row_ids).astype(F32).astype(BF16)
        hit = (turned[:ghosts] == row_ids[:ghosts] + blocks).astype(F32).astype(BF16)
        pt_halo[k * ghosts : (k + 1) * ghosts, :blocks] = hit
        pt_halo[k * ghosts : (k + 1) * ghosts, blocks:] = hit
    for pair in range(faces_n // 2):
        low = lane_ids < ghosts
        col = jnp.where(low, face_cols[2 * pair], face_cols[2 * pair + 1])
        want = jnp.where(low, lane_ids, lane_ids - ghosts) + blocks
        p_halo[:, pair * 2 * ghosts : (pair + 1) * 2 * ghosts] = (col == want).astype(F32).astype(BF16)
    wanted = jnp.concatenate(
        [send_ref[0, d : d + 1, :] for d in range(4)] + [jnp.full((1, blocks - ghosts), -1, jnp.int32)], axis=1
    )
    spread = jnp.broadcast_to(wanted, (blocks, blocks))
    pick_t[...] = (spread == row_ids).astype(F32).astype(BF16)[:, :ghosts]
    spread_t = jnp.transpose(spread.astype(F32)).astype(jnp.int32)
    pick[...] = (spread_t[:ghosts] == lane_ids[:ghosts]).astype(F32).astype(BF16)
    for k in range(slots):
        lift_t[:, k * nodes : (k + 1) * nodes] = jnp.transpose(lift_ref[k].astype(F32)).astype(BF16)
    row_ref[...] = jnp.zeros_like(row_ref)

    loads[0].wait()

    def lanes(c):
        return slice(c * nodes, (c + 1) * nodes)

    def target(shift):
        return (tm, jnp.clip(sp + shift, 0, n_space - 1))

    def inside(shift):
        return (sp + shift >= 0) & (sp + shift < n_space)

    def forward_copy(n, d):
        rows = pl.ds(d * halo, halo)
        return pltpu.make_async_remote_copy(
            src_ref=out_buf.at[n, rows], dst_ref=in_buf.at[n, rows],
            send_sem=send_sems.at[n, d], recv_sem=recv_sems.at[n, d],
            device_id=target(OFFSETS[d]), device_id_type=MESH,
        )

    def backward_copy(n, d):
        rows = pl.ds(d * halo, halo)
        return pltpu.make_async_remote_copy(
            src_ref=back_out.at[n, rows], dst_ref=back_in.at[n, rows],
            send_sem=bsend_sems.at[n, d], recv_sem=brecv_sems.at[n, d],
            device_id=target(-OFFSETS[d]), device_id_type=MESH,
        )

    def coef(k, e, c):
        return mixing_ref[(k * comps + e) * comps + c]

    def turn_of(level):
        angle = jnp.full((8, nodes), pitch_ref[level], F32)
        return jnp.cos(angle)[0:1], jnp.sin(angle)[0:1]

    pl.semaphore_wait(barrier, n_dev - 1)

    chunk = 32

    def forward(n, carry):
        level = tm * half + n
        active = (n < half - 1) | (tm == n_tm - 1)

        @pl.when(active)
        def _():
            for c in range(comps):
                sq_ref[:, lanes(c)] = jnp.tanh(u_ref[c]).astype(BF16)
            out_buf[n] = dot(pick[...], sq_ref[...]).astype(BF16)
            for d in range(4):
                @pl.when(inside(OFFSETS[d]))
                def _():
                    forward_copy(n, d).start()

        @pl.when(n == 0)
        def _():
            for load in loads[1:]:
                load.wait()

        keep = jnp.where(level > 0, 1.0, 0.0).astype(F32)
        for c in range(comps):
            state = u_ref[c]
            t = jnp.tanh(state)
            dd_ref[n, c] = STEP_SIZE * (1.0 - t * t)
            wu_ref[n, c] = (keep * weight_ref[c]) * state

        @pl.when(active)
        def _():
            cosine, sine = turn_of(level)
            squashed = sq_ref[...]
            for k in range(slots):
                if k == 0:
                    got = squashed
                else:
                    got = dot(p_own[(k - 1) * blocks : k * blocks, :], squashed).astype(BF16)
                stacked = jnp.concatenate([got[:, lanes(c)] for c in range(comps)], axis=0)
                y_ref[k] = dot(stacked, lift_t[:, lanes(k)])

            def own_mix(r, carry):
                start = pl.multiple_of(r * chunk, chunk)
                metric_half = STEP_SIZE * metric_ref[pl.ds(start, chunk), :]
                sums = [None] * comps
                for k in range(slots):
                    for c in range(comps):
                        term = y_ref[k, pl.ds(c * blocks + start, chunk), :]
                        for e in range(comps):
                            add = coef(k, e, c) * term
                            sums[e] = add if sums[e] is None else sums[e] + add
                for e in range(comps):
                    rows = pl.ds(start, chunk)
                    forcing = cosine * src_ref[0, e, rows, :] + sine * src_ref[1, e, rows, :]
                    base_ref[e, rows, :] = u_ref[e, rows, :] + STEP_SIZE * forcing - metric_half * sums[e]
                return carry

            lax.fori_loop(0, blocks // chunk, own_mix, 0)

            for d in range(4):
                @pl.when(inside(-OFFSETS[d]))
                def _():
                    forward_copy(n, d).wait_recv()

            ghost = in_buf[n]
            stacked = jnp.concatenate([ghost[:, lanes(c)] for c in range(comps)], axis=0)
            yh_ref[...] = dot(stacked, lift_t[:, nodes:])
            for k in range(1, slots):
                for part in range(ghosts // chunk):
                    for e in range(comps):
                        total = None
                        for c in range(comps):
                            at = c * ghosts + part * chunk
                            add = coef(k, e, c) * yh_ref[at : at + chunk, lanes(k - 1)]
                            total = add if total is None else total + add
                        at = (k - 1) * ghosts + part * chunk
                        z_ref[at : at + chunk, lanes(e)] = total.astype(BF16)
            more = dot(p_halo[...], z_ref[...])
            half_metric = STEP_SIZE * metric_ref[...]
            for e in range(comps):
                u_ref[e] = base_ref[e] - half_metric * more[:, lanes(e)]
            for d in range(4):
                @pl.when(inside(OFFSETS[d]))
                def _():
                    forward_copy(n, d).wait_send()

        return carry

    lax.fori_loop(0, half, forward, 0)

    def hand_copy():
        return pltpu.make_async_remote_copy(
            src_ref=a_ref, dst_ref=hand_ref, send_sem=hand_sems.at[0], recv_sem=hand_sems.at[1],
            device_id=(lax.rem(tm + n_tm - 1, n_tm), sp), device_id_type=MESH,
        )

    @pl.when(tm == n_tm - 1)
    def _():
        for c in range(comps):
            a_ref[c] = a_ref[c] + weight_ref[c] * u_ref[c]

    @pl.when(tm < n_tm - 1)
    def _():
        hand_copy().wait_recv()
        for c in range(comps):
            a_ref[c] = hand_ref[c]

    def grad_copy(r):
        other = lax.rem(me + r, n_dev)
        return pltpu.make_async_remote_copy(
            src_ref=row_ref, dst_ref=rows_ref.at[me], send_sem=gsend_sems.at[other], recv_sem=grecv_sems.at[me],
            device_id=(other // n_space, lax.rem(other, n_space)), device_id_type=MESH,
        )

    def backward(j, carry):
        n = half - 1 - j
        level = tm * half + n

        for e in range(comps):
            w = metric_ref[...] * a_ref[e]
            high = w.astype(BF16)
            sq_ref[:, lanes(e)] = high
            mixed_ref[0, :, lanes(e)] = (w - high.astype(F32)).astype(BF16)
        gw_ref[...] = dot(pt_halo[...], jnp.concatenate([sq_ref[...], mixed_ref[0]], axis=0))
        for k in range(1, slots):
            for part in range(ghosts // chunk):
                at = (k - 1) * ghosts + part * chunk
                for c in range(comps):
                    total = None
                    for e in range(comps):
                        add = coef(k, e, c) * gw_ref[at : at + chunk, lanes(e)]
                        total = add if total is None else total + add
                    to = c * ghosts + part * chunk
                    gh_ref[to : to + chunk, lanes(k - 1)] = total.astype(BF16)
        lifted = dot(gh_ref[...], lift_ref[1:].reshape(faces_n * nodes, nodes)).astype(BF16)
        for c in range(comps):
            back_out[n, :, lanes(c)] = lifted[c * ghosts : (c + 1) * ghosts]
        for d in range(4):
            @pl.when(inside(-OFFSETS[d]))
            def _():
                backward_copy(n, d).start()

        cosine, sine = turn_of(level)
        sums = None
        for e in range(comps):
            part = a_ref[e] * (cosine * src_ref[1, e] - sine * src_ref[0, e])
            sums = part if sums is None else sums + part
        value = jnp.sum(jnp.sum(sums, axis=0, keepdims=True), axis=1, keepdims=True) * (STEP_SIZE / norm)
        spots = lax.broadcasted_iota(jnp.int32, (1, nodes), 1)
        row_ref[...] = row_ref[...] + jnp.where(spots == level, value, 0.0)

        @pl.when(n == 0)
        def _():
            def tell(r, carry):
                grad_copy(r).start()
                return carry

            lax.fori_loop(1, n_dev, tell, 0)

        def own_mix(r, carry):
            start = pl.multiple_of(r * chunk, chunk)
            rows = pl.ds(start, chunk)
            weighted = [metric_ref[rows, :] * a_ref[e, rows, :] for e in range(comps)]
            for k in range(slots):
                for c in range(comps):
                    total = None
                    for e in range(comps):
                        add = coef(k, e, c) * weighted[e]
                        total = add if total is None else total + add
                    mixed_ref[k, rows, lanes(c)] = total.astype(BF16)
            return carry

        lax.fori_loop(0, blocks // chunk, own_mix, 0)
        for k in range(slots):
            if k == 0:
                got = mixed_ref[0]
            else:
                got = dot(pt_own[(k - 1) * blocks : k * blocks, :], mixed_ref[k]).astype(BF16)
            for c in range(comps):
                g_ref[c * blocks : (c + 1) * blocks, lanes(k)] = got[:, lanes(c)]
        pushed = dot(g_ref[...], lift_ref[...].reshape(slots * nodes, nodes))
        for c in range(comps):
            base_ref[c] = a_ref[c] + wu_ref[n, c] - dd_ref[n, c] * pushed[c * blocks : (c + 1) * blocks]

        for d in range(4):
            @pl.when(inside(OFFSETS[d]))
            def _():
                backward_copy(n, d).wait_recv()

        more = dot(pick_t[...], back_in[n])
        for c in range(comps):
            a_ref[c] = base_ref[c] - dd_ref[n, c] * more[:, lanes(c)]
        for d in range(4):
            @pl.when(inside(-OFFSETS[d]))
            def _():
                backward_copy(n, d).wait_send()
        return carry

    lax.fori_loop(0, half, backward, 0)

    @pl.when(tm > 0)
    def _():
        hand_copy().start()

    for c in range(comps):
        out_ref[0, c] = a_ref[c]

    def settle(r, carry):
        other = lax.rem(me + r, n_dev)
        pltpu.make_async_remote_copy(
            src_ref=row_ref, dst_ref=rows_ref.at[other], send_sem=gsend_sems.at[other],
            recv_sem=grecv_sems.at[other], device_id=(other // n_space, lax.rem(other, n_space)),
            device_id_type=MESH,
        ).wait()
        return carry

    lax.fori_loop(1, n_dev, settle, 0)
    rows_ref[me] = row_ref[...]
    grad_ref[...] = jnp.sum(rows_ref[...], axis=0)[:, : grad_ref.shape[1]]

    @pl.when(tm > 0)
    def _():
        hand_copy().wait_send()


def shards(
    checkpoints, sources, pitch, metric, obj_weight, adjoint_end, lift, mixing, faces, send_idx
):
    comps = sources.shape[1]
    blocks, nodes = metric.shape
    slots = lift.shape[0]
    halo = send_idx.shape[2]
    n_tm = lax.axis_size("tm")
    n_space = lax.axis_size("space")
    levels = pitch.shape[0]
    half = levels // n_tm
    ghosts = 4 * halo
    norm = math.sqrt(comps * nodes * blocks * n_space)
    wide = comps * nodes
    field = (comps, blocks, nodes)
    vmem = pl.BlockSpec(memory_space=pltpu.VMEM)
    smem = pl.BlockSpec(memory_space=pltpu.SMEM)
    anym = pl.BlockSpec(memory_space=pl.ANY)
    dma = pltpu.SemaphoreType.DMA
    n_dev = n_tm * n_space
    dims = (comps, blocks, nodes, slots, halo, half, n_tm, n_space, norm)
    bounds, grad = pl.pallas_call(
        functools.partial(window_kernel, dims),
        out_shape=(
            jax.ShapeDtypeStruct((1, *field), F32),
            jax.ShapeDtypeStruct((1, levels), F32),
        ),
        in_specs=[smem, smem, anym, anym, anym, anym, anym, vmem, vmem, vmem],
        out_specs=(vmem, vmem),
        scratch_shapes=[
            pltpu.VMEM(field, F32),
            pltpu.VMEM((2, *field), F32),
            pltpu.VMEM((blocks, nodes), F32),
            pltpu.VMEM(field, F32),
            pltpu.VMEM(field, F32),
            pltpu.VMEM(field, F32),
            pltpu.VMEM(field, F32),
            pltpu.VMEM((half, *field), F32),
            pltpu.VMEM((half, *field), F32),
            pltpu.VMEM((nodes, slots * nodes), BF16),
            pltpu.VMEM((blocks, wide), BF16),
            pltpu.VMEM(((slots - 1) * blocks, blocks), BF16),
            pltpu.VMEM((blocks, (slots - 1) * ghosts), BF16),
            pltpu.VMEM(((slots - 1) * blocks, blocks), BF16),
            pltpu.VMEM(((slots - 1) * ghosts, 2 * blocks), BF16),
            pltpu.VMEM((ghosts, blocks), BF16),
            pltpu.VMEM((blocks, ghosts), BF16),
            pltpu.VMEM((half, ghosts, wide), BF16),
            pltpu.VMEM((half, ghosts, wide), BF16),
            pltpu.VMEM((half, ghosts, wide), BF16),
            pltpu.VMEM((half, ghosts, wide), BF16),
            pltpu.VMEM((slots, comps * blocks, nodes), F32),
            pltpu.VMEM((comps * ghosts, (slots - 1) * nodes), F32),
            pltpu.VMEM(((slots - 1) * ghosts, wide), BF16),
            pltpu.VMEM((slots, blocks, wide), BF16),
            pltpu.VMEM((comps * blocks, slots * nodes), BF16),
            pltpu.VMEM(((slots - 1) * ghosts, wide), F32),
            pltpu.VMEM((comps * ghosts, (slots - 1) * nodes), BF16),
            pltpu.VMEM((1, nodes), F32),
            pltpu.VMEM((n_dev, 1, nodes), F32),
            dma((5,)),
            dma((half, 4)),
            dma((half, 4)),
            dma((half, 4)),
            dma((half, 4)),
            dma((2,)),
            dma((n_dev,)),
            dma((n_dev,)),
        ],
        compiler_params=pltpu.CompilerParams(
            collective_id=0, has_side_effects=True, vmem_limit_bytes=48 * 1024 * 1024
        ),
        name="window",
    )(pitch, mixing.reshape(-1), checkpoints, sources, metric, obj_weight, adjoint_end, lift, faces, send_idx)
    return bounds, grad.reshape(-1)


def solution(mesh):
    placed = (
        P("tm", None, "space", None),
        P(None, None, "space", None),
        P(),
        P("space", None),
        P(None, "space", None),
        P(None, "space", None),
        P(),
        P(),
        P("space", None),
        P("space", None, None),
    )
    return jax.shard_map(
        shards,
        mesh=mesh,
        in_specs=placed,
        out_specs=(P("tm", None, "space", None), P()),
        check_vma=False,
    )
```

```python
import functools
import math

import jax
import jax.numpy as jnp
from jax import lax
from jax.experimental import pallas as pl
from jax.experimental.pallas import tpu as pltpu
from jax.sharding import PartitionSpec as P

OFFSETS = (1, -1, 2, -2)
STEP_SIZE = 0.5
F32 = jnp.float32
BF16 = jnp.bfloat16
MESH = pl.DeviceIdType.MESH


def dot(a, b):
    return jnp.dot(a, b, preferred_element_type=F32)


def window_kernel(
    dims,
    pitch_ref, mixing_ref, cp_hbm, src_hbm, metric_hbm, weight_hbm, end_hbm, lift_hbm, faces_hbm, send_hbm,
    out_ref, grad_ref,
    u_ref, lift_ref, faces_ref, send_ref, src_ref, metric_ref, weight_ref, a_ref, hand_ref, base_ref, dd_ref, wu_ref, lift_t, sq_ref,
    p_own, p_halo, pt_own, pt_halo, pick, pick_t, out_buf, in_buf, back_out, back_in, y_ref, yh_ref, z_ref,
    mixed_ref, g_ref, gw_ref, gh_ref, row_ref, rows_ref,
    load_sems, send_sems, recv_sems, bsend_sems, brecv_sems, hand_sems, factor_sems, gsend_sems, grecv_sems,
):
    comps, blocks, nodes, slots, halo, half, n_tm, n_space, norm = dims
    ghosts = 4 * halo
    faces_n = slots - 1
    wide = comps * nodes
    tm = lax.axis_index("tm")
    sp = lax.axis_index("space")
    n_dev = n_tm * n_space
    me = tm * n_space + sp
    lead = tm == n_tm - 1
    partner = (n_tm - 1 - tm, sp)
    segment = tm
    levels = half * n_tm

    loads = [
        pltpu.make_async_copy(send_hbm, send_ref, load_sems.at[5]),
        pltpu.make_async_copy(faces_hbm, faces_ref, load_sems.at[6]),
        pltpu.make_async_copy(cp_hbm.at[0], u_ref, load_sems.at[0]),
        pltpu.make_async_copy(lift_hbm, lift_ref, load_sems.at[7]),
        pltpu.make_async_copy(src_hbm, src_ref, load_sems.at[1]),
        pltpu.make_async_copy(metric_hbm, metric_ref, load_sems.at[2]),
        pltpu.make_async_copy(weight_hbm, weight_ref, load_sems.at[3]),
        pltpu.make_async_copy(end_hbm, a_ref, load_sems.at[4]),
    ]
    for load in loads:
        load.start()

    in_buf[...] = jnp.zeros_like(in_buf)
    back_in[...] = jnp.zeros_like(back_in)

    barrier = pltpu.get_barrier_semaphore()

    def greet(r, carry):
        other = lax.rem(me + r, n_dev)
        pl.semaphore_signal(
            barrier, inc=1, device_id=(other // n_space, lax.rem(other, n_space)), device_id_type=MESH
        )
        return carry

    lax.fori_loop(1, n_dev, greet, 0)

    for load in loads[:2]:
        load.wait()
    row_ids = lax.broadcasted_iota(jnp.int32, (blocks, blocks), 0)
    lane_ids = lax.broadcasted_iota(jnp.int32, (blocks, blocks), 1)
    face_cols = []
    for k in range(faces_n):
        turned = jnp.broadcast_to(faces_ref[k : k + 1, :], (blocks, blocks))
        col = jnp.transpose(turned.astype(F32)).astype(jnp.int32)
        face_cols.append(col)
        p_own[k * blocks : (k + 1) * blocks, :] = (col == lane_ids).astype(F32).astype(BF16)
        pt_own[k * blocks : (k + 1) * blocks, :] = (turned == row_ids).astype(F32).astype(BF16)
        hit = (turned[:ghosts] == row_ids[:ghosts] + blocks).astype(F32).astype(BF16)
        pt_halo[k * ghosts : (k + 1) * ghosts, :blocks] = hit
        pt_halo[k * ghosts : (k + 1) * ghosts, blocks:] = hit
    for pair in range(faces_n // 2):
        low = lane_ids < ghosts
        col = jnp.where(low, face_cols[2 * pair], face_cols[2 * pair + 1])
        want = jnp.where(low, lane_ids, lane_ids - ghosts) + blocks
        p_halo[:, pair * 2 * ghosts : (pair + 1) * 2 * ghosts] = (col == want).astype(F32).astype(BF16)
    wanted = jnp.concatenate(
        [send_ref[0, d : d + 1, :] for d in range(4)] + [jnp.full((1, blocks - ghosts), -1, jnp.int32)], axis=1
    )
    spread = jnp.broadcast_to(wanted, (blocks, blocks))
    pick_t[...] = (spread == row_ids).astype(F32).astype(BF16)[:, :ghosts]
    spread_t = jnp.transpose(spread.astype(F32)).astype(jnp.int32)
    pick[...] = (spread_t[:ghosts] == lane_ids[:ghosts]).astype(F32).astype(BF16)
    row_ref[...] = jnp.zeros_like(row_ref)
    loads[2].wait()

    def lanes(c):
        return slice(c * nodes, (c + 1) * nodes)

    def target(shift):
        return (tm, jnp.clip(sp + shift, 0, n_space - 1))

    def inside(shift):
        return (sp + shift >= 0) & (sp + shift < n_space)

    def forward_copy(n, d):
        rows = pl.ds(d * halo, halo)
        return pltpu.make_async_remote_copy(
            src_ref=out_buf.at[n, rows], dst_ref=in_buf.at[n, rows],
            send_sem=send_sems.at[n, d], recv_sem=recv_sems.at[n, d],
            device_id=target(OFFSETS[d]), device_id_type=MESH,
        )

    def backward_copy(n, d):
        rows = pl.ds(d * halo, halo)
        return pltpu.make_async_remote_copy(
            src_ref=back_out.at[n, rows], dst_ref=back_in.at[n, rows],
            send_sem=bsend_sems.at[n, d], recv_sem=brecv_sems.at[n, d],
            device_id=target(-OFFSETS[d]), device_id_type=MESH,
        )

    def coef(k, e, c):
        return mixing_ref[k, e, c]

    def turn_of(level):
        angle = jnp.full((8, nodes), pitch_ref[level], F32)
        return jnp.cos(angle)[0:1], jnp.sin(angle)[0:1]

    for c in range(comps):
        sq_ref[:, lanes(c)] = jnp.tanh(u_ref[c]).astype(BF16)
    out_buf[0] = dot(pick[...], sq_ref[...]).astype(BF16)
    pl.semaphore_wait(barrier, n_dev - 1)
    for d in range(4):
        @pl.when(inside(OFFSETS[d]))
        def _():
            forward_copy(0, d).start()

    chunk = 32
    for load in loads[3:]:
        load.wait()
    for k in range(slots):
        lift_t[:, k * nodes : (k + 1) * nodes] = jnp.transpose(lift_ref[k].astype(F32)).astype(BF16)

    def factor_copy(level, which):
        ref = (dd_ref, wu_ref)[which]
        return pltpu.make_async_remote_copy(
            src_ref=ref.at[level], dst_ref=ref.at[level], send_sem=factor_sems.at[0, which, level],
            recv_sem=factor_sems.at[1, which, level], device_id=partner, device_id_type=MESH,
        )

    def forward(n, carry):
        level = segment * half + n
        active = (n < half - 1) | lead

        @pl.when(active & (n > 0))
        def _():
            for c in range(comps):
                sq_ref[:, lanes(c)] = jnp.tanh(u_ref[c]).astype(BF16)
            out_buf[n] = dot(pick[...], sq_ref[...]).astype(BF16)
            for d in range(4):
                @pl.when(inside(OFFSETS[d]))
                def _():
                    forward_copy(n, d).start()

        keep = jnp.where(level > 0, 1.0, 0.0).astype(F32)
        for c in range(comps):
            state = u_ref[c]
            t = jnp.tanh(state)
            dd_ref[level, c] = STEP_SIZE * (1.0 - t * t)
            wu_ref[level, c] = (keep * weight_ref[c]) * state

        @pl.when(jnp.logical_not(lead))
        def _():
            factor_copy(level, 0).start()
            factor_copy(level, 1).start()

        @pl.when(active)
        def _():
            cosine, sine = turn_of(level)
            squashed = sq_ref[...]
            for k in range(slots):
                if k == 0:
                    got = squashed
                else:
                    got = dot(p_own[(k - 1) * blocks : k * blocks, :], squashed).astype(BF16)
                stacked = jnp.concatenate([got[:, lanes(c)] for c in range(comps)], axis=0)
                y_ref[k] = dot(stacked, lift_t[:, lanes(k)])

            def own_mix(r, carry):
                start = pl.multiple_of(r * chunk, chunk)
                metric_half = STEP_SIZE * metric_ref[pl.ds(start, chunk), :]
                sums = [None] * comps
                for k in range(slots):
                    for c in range(comps):
                        term = y_ref[k, pl.ds(c * blocks + start, chunk), :]
                        for e in range(comps):
                            add = coef(k, e, c) * term
                            sums[e] = add if sums[e] is None else sums[e] + add
                for e in range(comps):
                    rows = pl.ds(start, chunk)
                    forcing = cosine * src_ref[0, e, rows, :] + sine * src_ref[1, e, rows, :]
                    base_ref[e, rows, :] = u_ref[e, rows, :] + STEP_SIZE * forcing - metric_half * sums[e]
                return carry

            lax.fori_loop(0, blocks // chunk, own_mix, 0)

            for d in range(4):
                @pl.when(inside(-OFFSETS[d]))
                def _():
                    forward_copy(n, d).wait_recv()

            ghost = in_buf[n]
            stacked = jnp.concatenate([ghost[:, lanes(c)] for c in range(comps)], axis=0)
            yh_ref[...] = dot(stacked, lift_t[:, nodes:])
            for k in range(1, slots):
                for part in range(ghosts // chunk):
                    for e in range(comps):
                        total = None
                        for c in range(comps):
                            at = c * ghosts + part * chunk
                            add = coef(k, e, c) * yh_ref[at : at + chunk, lanes(k - 1)]
                            total = add if total is None else total + add
                        at = (k - 1) * ghosts + part * chunk
                        z_ref[at : at + chunk, lanes(e)] = total.astype(BF16)
            more = dot(p_halo[...], z_ref[...])
            half_metric = STEP_SIZE * metric_ref[...]
            for e in range(comps):
                u_ref[e] = base_ref[e] - half_metric * more[:, lanes(e)]
            for d in range(4):
                @pl.when(inside(OFFSETS[d]))
                def _():
                    forward_copy(n, d).wait_send()

        return carry

    lax.fori_loop(0, half, forward, 0)

    def hand_copy():
        return pltpu.make_async_remote_copy(
            src_ref=a_ref, dst_ref=out_ref.at[0], send_sem=hand_sems.at[0], recv_sem=hand_sems.at[1],
            device_id=partner, device_id_type=MESH,
        )

    def keep_copy():
        return pltpu.make_async_copy(hand_ref, out_ref.at[0], hand_sems.at[2])

    def grad_copy(source, other):
        return pltpu.make_async_remote_copy(
            src_ref=row_ref, dst_ref=rows_ref.at[source], send_sem=gsend_sems.at[other],
            recv_sem=grecv_sems.at[source], device_id=(other // n_space, lax.rem(other, n_space)),
            device_id_type=MESH,
        )

    def backward(j, carry):
        level = levels - 1 - j
        n = level

        for e in range(comps):
            w = metric_ref[...] * a_ref[e]
            high = w.astype(BF16)
            sq_ref[:, lanes(e)] = high
            mixed_ref[0, :, lanes(e)] = (w - high.astype(F32)).astype(BF16)
        gw_ref[...] = dot(pt_halo[...], jnp.concatenate([sq_ref[...], mixed_ref[0]], axis=0))
        for k in range(1, slots):
            for part in range(ghosts // chunk):
                at = (k - 1) * ghosts + part * chunk
                for c in range(comps):
                    total = None
                    for e in range(comps):
                        add = coef(k, e, c) * gw_ref[at : at + chunk, lanes(e)]
                        total = add if total is None else total + add
                    to = c * ghosts + part * chunk
                    gh_ref[to : to + chunk, lanes(k - 1)] = total.astype(BF16)
        lifted = dot(gh_ref[...], lift_ref[1:].reshape(faces_n * nodes, nodes)).astype(BF16)
        for c in range(comps):
            back_out[n, :, lanes(c)] = lifted[c * ghosts : (c + 1) * ghosts]
        for d in range(4):
            @pl.when(inside(-OFFSETS[d]))
            def _():
                backward_copy(n, d).start()

        @pl.when(level < half)
        def _():
            factor_copy(level, 0).wait_recv()
            factor_copy(level, 1).wait_recv()

        cosine, sine = turn_of(level)
        sums = None
        for e in range(comps):
            part = a_ref[e] * (cosine * src_ref[1, e] - sine * src_ref[0, e])
            sums = part if sums is None else sums + part
        value = jnp.sum(jnp.sum(sums, axis=0, keepdims=True), axis=1, keepdims=True) * (STEP_SIZE / norm)
        spots = lax.broadcasted_iota(jnp.int32, (1, nodes), 1)
        row_ref[...] = row_ref[...] + jnp.where(spots == level, value, 0.0)

        @pl.when(n == 0)
        def _():
            def tell(r, carry):
                grad_copy(sp, lax.rem(me + r, n_dev)).start()
                return carry

            lax.fori_loop(1, n_dev, tell, 0)

        def own_mix(r, carry):
            start = pl.multiple_of(r * chunk, chunk)
            rows = pl.ds(start, chunk)
            weighted = [metric_ref[rows, :] * a_ref[e, rows, :] for e in range(comps)]
            for k in range(slots):
                for c in range(comps):
                    total = None
                    for e in range(comps):
                        add = coef(k, e, c) * weighted[e]
                        total = add if total is None else total + add
                    mixed_ref[k, rows, lanes(c)] = total.astype(BF16)
            return carry

        lax.fori_loop(0, blocks // chunk, own_mix, 0)
        for k in range(slots):
            if k == 0:
                got = mixed_ref[0]
            else:
                got = dot(pt_own[(k - 1) * blocks : k * blocks, :], mixed_ref[k]).astype(BF16)
            for c in range(comps):
                g_ref[c * blocks : (c + 1) * blocks, lanes(k)] = got[:, lanes(c)]
        pushed = dot(g_ref[...], lift_ref[...].reshape(slots * nodes, nodes))
        for c in range(comps):
            base_ref[c] = a_ref[c] + wu_ref[n, c] - dd_ref[n, c] * pushed[c * blocks : (c + 1) * blocks]

        for d in range(4):
            @pl.when(inside(OFFSETS[d]))
            def _():
                backward_copy(n, d).wait_recv()

        more = dot(pick_t[...], back_in[n])
        for c in range(comps):
            a_ref[c] = base_ref[c] - dd_ref[n, c] * more[:, lanes(c)]
        for d in range(4):
            @pl.when(inside(-OFFSETS[d]))
            def _():
                backward_copy(n, d).wait_send()

        @pl.when(level == half)
        def _():
            for c in range(comps):
                hand_ref[c] = a_ref[c]
            keep_copy().start()

        return carry

    @pl.when(lead)
    def _():
        for c in range(comps):
            a_ref[c] = a_ref[c] + weight_ref[c] * u_ref[c]
        lax.fori_loop(0, levels, backward, 0)
        hand_copy().start()
        rows_ref[sp] = row_ref[...]

        def settle(r, carry):
            other = lax.rem(sp + r, n_space)
            grad_copy(other, me).wait_recv()
            return carry

        lax.fori_loop(1, n_space, settle, 0)

    @pl.when(jnp.logical_not(lead))
    def _():
        def settle(r, carry):
            grad_copy(r, me).wait_recv()
            return carry

        lax.fori_loop(0, n_space, settle, 0)

    grad_ref[...] = jnp.sum(rows_ref[...], axis=0)[0, : grad_ref.shape[0]]

    @pl.when(lead)
    def _():
        hand_copy().wait_send()
        keep_copy().wait()

        def sent(r, carry):
            grad_copy(sp, lax.rem(me + r, n_dev)).wait_send()
            return carry

        lax.fori_loop(1, n_dev, sent, 0)

    @pl.when(jnp.logical_not(lead))
    def _():
        hand_copy().wait_recv()
        for level in range(half):
            factor_copy(level, 0).wait_send()
            factor_copy(level, 1).wait_send()


def shards(
    checkpoints, sources, pitch, metric, obj_weight, adjoint_end, lift, mixing, faces, send_idx
):
    comps = sources.shape[1]
    blocks, nodes = metric.shape
    slots = lift.shape[0]
    halo = send_idx.shape[2]
    n_tm = lax.axis_size("tm")
    n_space = lax.axis_size("space")
    levels = pitch.shape[0]
    half = levels // n_tm
    ghosts = 4 * halo
    norm = math.sqrt(comps * nodes * blocks * n_space)
    wide = comps * nodes
    field = (comps, blocks, nodes)
    vmem = pl.BlockSpec(memory_space=pltpu.VMEM)
    smem = pl.BlockSpec(memory_space=pltpu.SMEM)
    anym = pl.BlockSpec(memory_space=pl.ANY)
    dma = pltpu.SemaphoreType.DMA
    n_dev = n_tm * n_space
    dims = (comps, blocks, nodes, slots, halo, half, n_tm, n_space, norm)
    bounds, grad = pl.pallas_call(
        functools.partial(window_kernel, dims),
        out_shape=(
            jax.ShapeDtypeStruct((1, *field), F32),
            jax.ShapeDtypeStruct((levels,), F32),
        ),
        in_specs=[smem, smem] + [anym] * 8,
        out_specs=(anym, vmem),
        scratch_shapes=[
            pltpu.VMEM(field, F32),
            pltpu.VMEM(lift.shape, BF16),
            pltpu.VMEM(faces.shape[::-1], jnp.int32),
            pltpu.VMEM(send_idx.shape, jnp.int32),
            pltpu.VMEM((2, *field), F32),
            pltpu.VMEM((blocks, nodes), F32),
            pltpu.VMEM(field, F32),
            pltpu.VMEM(field, F32),
            pltpu.VMEM(field, F32),
            pltpu.VMEM(field, F32),
            pltpu.VMEM((levels, *field), F32),
            pltpu.VMEM((levels, *field), F32),
            pltpu.VMEM((nodes, slots * nodes), BF16),
            pltpu.VMEM((blocks, wide), BF16),
            pltpu.VMEM(((slots - 1) * blocks, blocks), BF16),
            pltpu.VMEM((blocks, (slots - 1) * ghosts), BF16),
            pltpu.VMEM(((slots - 1) * blocks, blocks), BF16),
            pltpu.VMEM(((slots - 1) * ghosts, 2 * blocks), BF16),
            pltpu.VMEM((ghosts, blocks), BF16),
            pltpu.VMEM((blocks, ghosts), BF16),
            pltpu.VMEM((half, ghosts, wide), BF16),
            pltpu.VMEM((half, ghosts, wide), BF16),
            pltpu.VMEM((levels, ghosts, wide), BF16),
            pltpu.VMEM((levels, ghosts, wide), BF16),
            pltpu.VMEM((slots, comps * blocks, nodes), F32),
            pltpu.VMEM((comps * ghosts, (slots - 1) * nodes), F32),
            pltpu.VMEM(((slots - 1) * ghosts, wide), BF16),
            pltpu.VMEM((slots, blocks, wide), BF16),
            pltpu.VMEM((comps * blocks, slots * nodes), BF16),
            pltpu.VMEM(((slots - 1) * ghosts, wide), F32),
            pltpu.VMEM((comps * ghosts, (slots - 1) * nodes), BF16),
            pltpu.VMEM((1, nodes), F32),
            pltpu.VMEM((n_space, 1, nodes), F32),
            dma((8,)),
            dma((half, 4)),
            dma((half, 4)),
            dma((levels, 4)),
            dma((levels, 4)),
            dma((3,)),
            dma((2, 2, half)),
            dma((n_dev,)),
            dma((n_space,)),
        ],
        compiler_params=pltpu.CompilerParams(
            collective_id=0, has_side_effects=True, vmem_limit_bytes=60 * 1024 * 1024
        ),
        name="window",
    )(pitch, mixing, checkpoints, sources, metric, obj_weight, adjoint_end, lift, faces.T, send_idx)
    return bounds, grad


def solution(mesh):
    placed = (
        P("tm", None, "space", None),
        P(None, None, "space", None),
        P(),
        P("space", None),
        P(None, "space", None),
        P(None, "space", None),
        P(),
        P(),
        P("space", None),
        P("space", None, None),
    )
    return jax.shard_map(
        shards,
        mesh=mesh,
        in_specs=placed,
        out_specs=(P("tm", None, "space", None), P()),
        check_vma=False,
    )
```
